128 devices in a mesh: fsdp: 8 (over x, y_lo), tensor: 16 (over z, y_hi, core).
Axes of the slice: x: 4, y: 4 (y_hi: 2, y_lo: 2; y = y_hi * 2 + y_lo), z: 4, core: 2. Of those that a mesh axis runs over, the one named last changes fastest.
Arguments:
- modality: int32 [8192], P('fsdp'), may hold values from 0 to 2, as said below
- out_grad: bfloat16 [8192, 4096], P('fsdp', 'tensor'), may hold values from -6 to 6
- gate_pre: bfloat16 [8192, 11008], P('fsdp', 'tensor'), may hold values from -6 to 6
- up_pre: bfloat16 [8192, 11008], P('fsdp', 'tensor'), may hold values from -6 to 6
- down_weight: bfloat16 [3, 11008, 4096], P(None, 'tensor', 'fsdp'), may hold values from -0.0546875 to 0.0546875
Outputs:
- down_grad: float32 [3, 11008, 4096], P(None, 'tensor', 'fsdp')
- gate_grad: bfloat16 [8192, 11008], P('fsdp', 'tensor')
- up_grad: bfloat16 [8192, 11008], P('fsdp', 'tensor')
The draws below stay inside these ranges and needn't reach their ends.
Inputs may be any that keep to these rules, and one draw needn't show every extreme that they name: `modality`: the 1024 tokens of every index of fsdp hold each of the three modalities at least once.
All inputs are finite; a program needn't handle non-finite values.
Results may differ from the reference program's by a relative error of at most 0.012.
Values may be sent and summed in bfloat16 or wider, within the bound.
No kernel may reach another device: no remote copies, remote signals or barrier semaphores. Data moves between devices by JAX's collectives and lax.ppermute only.
A program may use at most 256 MiB of HBM per device.

```python
import jax
import jax.numpy as jnp
from jax import lax

D = 4096
FF = 11008
TOK_DEV = 1024
TOKENS = 8192
N_FSDP = 8


def draw_modality(key, part):
    subkeys = jax.random.split(jax.random.fold_in(key, 11), 4)
    groups = TOKENS // TOK_DEV
    position = jnp.arange(TOKENS, dtype=jnp.int32)
    group_id = position // TOK_DEV
    local_pos = position % TOK_DEV
    rotation = jax.random.randint(subkeys[0], (), 0, 3)
    leader = (jnp.arange(groups, dtype=jnp.int32) + rotation) % 3
    shares = jax.random.randint(subkeys[1], (groups,), 3, 9)
    offsets = jax.random.randint(subkeys[2], (groups,), 0, TOK_DEV)
    rolls = jax.random.randint(subkeys[3], (TOKENS,), 0, 20)
    lead_kind = leader[group_id]
    base_kind = jnp.where(rolls < 2 * shares[group_id], lead_kind, (lead_kind + 1 + rolls % 2) % 3)
    distance = (local_pos - offsets[group_id]) % TOK_DEV
    return jnp.where(distance < 3, distance, base_kind).astype(jnp.int32)


def spiked(entries, stream_key, source, target, shards_of, factor):
    owner, partner = [(jnp.arange(entries.shape[axis_at]) // (entries.shape[axis_at] // shards_of)).reshape([-1 if axis == axis_at else 1 for axis in range(entries.ndim)]) for axis_at in (source, target)]
    chosen = jax.random.permutation(stream_key, shards_of)[partner]
    strong = (owner == chosen) | (owner == (partner + shards_of // 2) % shards_of)
    return jnp.where(strong, factor * entries, entries)


def block_scale(rng, shape, pieces, smallest, high):
    def one(dim, shards_of):
        heights = jax.random.uniform(jax.random.fold_in(jax.random.fold_in(rng, 6), dim), (shards_of,), jnp.float32, smallest / len(pieces), high / len(pieces))
        return jnp.repeat(jnp.exp(heights), shape[dim] // shards_of).reshape((-1,) + (1,) * (len(shape) - dim - 1))

    factor_of = one(*pieces[0])
    for cut in pieces[1:]:
        factor_of = factor_of * one(*cut)
    return factor_of


def gaussian(stream_key, shape, deviation, bound, cuts=(), kind=jnp.bfloat16):
    loudness = block_scale(stream_key, shape, cuts, -0.22, 0.18) if cuts else 1.0
    drawn = jax.random.normal(stream_key, shape, jnp.float32) * deviation * loudness
    return jnp.minimum(jnp.maximum(drawn, -bound), bound).astype(kind)


def gaussian_with(own_key, dims, width, bound, cuts, heavy, kind=jnp.bfloat16):
    array = width * jax.random.normal(own_key, dims, jnp.float32)
    if cuts:
        array = array * block_scale(own_key, dims, cuts, -0.22, 0.18)
    return jnp.clip(spiked(array, jax.random.fold_in(own_key, 3), *heavy), -bound, bound).astype(kind)


def setup_inputs(seed: int = 0) -> dict:
    keys = jax.random.split(jax.random.key(seed), 6)
    modality = draw_modality(jax.random.fold_in(keys[5], 71), 0)
    out_grad = gaussian_with(keys[1], (TOKENS, D), 1.0, 6.0, ((0, 8), (1, 16)), (0, 1, 16, 2.0))
    gate_pre = gaussian(keys[2], (TOKENS, FF), 1.0, 6.0, ((0, 8), (1, 16)))
    up_pre = gaussian(keys[3], (TOKENS, FF), 1.0, 6.0, ((0, 8), (1, 16)))
    down_weight = gaussian(keys[4], (3, FF, D), FF ** -0.5, 0.0546875, ((1, 16), (2, 8)))
    return dict(modality=modality, out_grad=out_grad, gate_pre=gate_pre, up_pre=up_pre, down_weight=down_weight)


def reference(modality, out_grad, gate_pre, up_pre, down_weight):
    labels = jnp.arange(3, dtype=jnp.int32)
    kind_onehot = (modality[:, None] == labels[None, :]).astype(jnp.float32)
    counts = jnp.sum(kind_onehot, axis=0)
    factor = TOKENS / (3.0 * counts)
    token_scale = jnp.sum(kind_onehot * factor[None, :], axis=1)
    scaled = (out_grad.astype(jnp.float32) * token_scale[:, None]).astype(jnp.bfloat16)
    gate_val = gate_pre.astype(jnp.float32)
    up_val = up_pre.astype(jnp.float32)
    sigmoid_g = jax.nn.sigmoid(gate_val)
    active = gate_val * sigmoid_g
    hidden = (active * up_val).astype(jnp.bfloat16)
    kind_marks = kind_onehot.T.astype(jnp.bfloat16)
    d_hidden = jnp.zeros((TOKENS, FF), jnp.float32)
    for kind_id in range(3):
        masked = scaled * kind_marks[kind_id][:, None]
        d_hidden = d_hidden + lax.dot_general(masked, down_weight[kind_id], (((1,), (1,)), ((), ())), preferred_element_type=jnp.float32)
    up_grad = (d_hidden * active).astype(jnp.bfloat16)
    slope = sigmoid_g * (1.0 + gate_val * (1.0 - sigmoid_g))
    gate_grad = (d_hidden * up_val * slope).astype(jnp.bfloat16)
    group_hidden = hidden.reshape(N_FSDP, TOK_DEV, FF)
    group_scaled = scaled.reshape(N_FSDP, TOK_DEV, D)
    group_marks = jnp.transpose(kind_marks.reshape(3, N_FSDP, TOK_DEV), (1, 0, 2))

    def one_group(running, group_items):
        rows_hidden, rows_scaled, marks_here = group_items
        partials = []
        for kind_id in range(3):
            masked = rows_scaled * marks_here[kind_id][:, None]
            product = lax.dot_general(rows_hidden, masked, (((0,), (0,)), ((), ())), preferred_element_type=jnp.float32)
            partials.append(lax.optimization_barrier(product.astype(jnp.bfloat16)).astype(jnp.float32))
        return running + jnp.stack(partials), None

    down_grad, _ = lax.scan(one_group, jnp.zeros((3, FF, D), jnp.float32), (group_hidden, group_scaled, group_marks))
    return down_grad, gate_grad, up_grad
```

```python
import jax
import jax.numpy as jnp
from jax import lax
from jax.experimental import pallas as pl
from jax.experimental.pallas import tpu as pltpu
from jax.sharding import Mesh
from jax.sharding import PartitionSpec as P


ANY = pl.ANY
VM = pltpu.VMEM
BF = jnp.bfloat16
F32 = jnp.float32
NX = 4
LIMIT = 60 * 1024 * 1024


def moved(value, axis, step):
    return lax.ppermute(value, axis, [(i, (i + step) % NX) for i in range(NX)])


def swapped(value, axis):
    return lax.ppermute(value, axis, [(0, 1), (1, 0)])


def nt(a, b):
    return lax.dot_general(a, b, (((1,), (1,)), ((), ())), preferred_element_type=F32)


def nn(a, b):
    return lax.dot_general(a, b, (((1,), (0,)), ((), ())), preferred_element_type=F32)


def hidden_half(gate, up, half):
    tok, hid = gate.shape
    tile = tok // 4

    def body(g_ref, u_ref, o_ref):
        g = g_ref[...].astype(F32)
        h = (g * jax.nn.sigmoid(g) * u_ref[...].astype(F32)).astype(BF)
        o_ref[...] = h.T

    spec = pl.BlockSpec((tile, hid), lambda i: (2 * half + i, 0))
    return pl.pallas_call(
        body,
        grid=(2,),
        in_specs=[spec, spec],
        out_specs=pl.BlockSpec((hid, tile), lambda i: (0, i)),
        out_shape=jax.ShapeDtypeStruct((hid, tok // 2), BF),
        name=f"hid{half}",
        cost_estimate=pl.CostEstimate(flops=2_000_000_000, bytes_accessed=2 * tok * hid, transcendentals=0),
    )(gate, up)


def d_hidden_slots(w_own, w_other, pieces, mods, slots, name):
    kinds, hid, width = w_own.shape
    tok = pieces[0].shape[0]
    quarter = pieces[0].shape[1]
    half = tok // 2
    tile = 256

    def body(*refs):
        w_refs = refs[:2]
        x_refs = refs[2:18]
        mod_ref = refs[18]
        outs = refs[19:-4]
        w_s, x_s, w_sem, x_sem = refs[-4:]
        x, yl, z, yh, core = (lax.axis_index(a) for a in ("x", "yl", "z", "yh", "core"))

        def x_copies(n, r):
            return [
                pltpu.make_async_copy(
                    x_refs[r * 4 + a * 2 + b],
                    x_s.at[n, :, pl.ds(pl.multiple_of((yh ^ a) * 2 * quarter + (core ^ b) * quarter, quarter), quarter)],
                    x_sem.at[n, a * 2 + b],
                )
                for a in range(2)
                for b in range(2)
            ]

        for n, j in enumerate(slots):
            rel = (x + j + NX - z) % NX
            for r in range(NX):

                @pl.when(rel == r)
                def _(n=n, r=r):
                    for c in x_copies(n, r):
                        c.start()

        w_copies = [
            [
                pltpu.make_async_copy(
                    w_refs[s].at[m],
                    w_s.at[m, :, pl.ds(pl.multiple_of((yl ^ s) * width, width), width)],
                    w_sem.at[m, s],
                )
                for s in range(2)
            ]
            for m in range(kinds)
        ]
        for pair in w_copies:
            for c in pair:
                c.start()
        for n, j in enumerate(slots):
            for c in x_copies(n, 0):
                c.wait()
            for t in range(tok // tile):
                xt = x_s[n, t * tile : (t + 1) * tile, :]
                row = mod_ref[:, j * tok + t * tile : j * tok + (t + 1) * tile]
                total = None
                for m in range(kinds):
                    if n == 0 and t == 0:
                        for c in w_copies[m]:
                            c.wait()
                    part = nt(w_s[m], xt)
                    total = part if total is None else jnp.where(row == m, part, total)
                if j == 0:
                    outs[-1][:, t * tile : (t + 1) * tile] = total
                else:
                    o = outs[2 * n + (t * tile) // half]
                    start = (t * tile) % half
                    o[:, start : start + tile] = total.astype(BF)

    out_shape = []
    for j in slots:
        if j == 0:
            out_shape.append(jax.ShapeDtypeStruct((hid, tok), F32))
        else:
            out_shape += [jax.ShapeDtypeStruct((hid, half), BF)] * 2
    flops = 2 * len(slots) * kinds * tok * hid * 2 * width
    return pl.pallas_call(
        body,
        in_specs=[pl.BlockSpec(memory_space=ANY)] * 18 + [pl.BlockSpec(memory_space=VM)],
        out_specs=[pl.BlockSpec(memory_space=VM)] * len(out_shape),
        out_shape=out_shape,
        scratch_shapes=[
            VM((kinds, hid, 2 * width), BF),
            VM((len(slots), tok, 2 * width), BF),
            pltpu.SemaphoreType.DMA((kinds, 2)),
            pltpu.SemaphoreType.DMA((len(slots), 4)),
        ],
        compiler_params=pltpu.CompilerParams(vmem_limit_bytes=LIMIT),
        name=name,
        cost_estimate=pl.CostEstimate(flops=flops, bytes_accessed=0, transcendentals=0),
    )(w_own, w_other, *pieces, mods)


def weight_grad(hid_halves, pieces, mods, mine):
    hid, half = hid_halves[0].shape
    quarter = pieces[0].shape[1]
    tok = pieces[0].shape[0]
    kinds = 3
    dtype = F32 if mine else BF

    def body(*refs):
        h_refs = refs[:8]
        x_refs = refs[8:24]
        mod_ref = refs[24]
        o_ref, h_s, x_s, h_sem, x_sem = refs[25:]
        x, yl, z, yh, core = (lax.axis_index(a) for a in ("x", "yl", "z", "yh", "core"))
        side = yl if mine else 1 - yl
        h_copies = [
            pltpu.make_async_copy(h_refs[i], h_s.at[:, pl.ds(i * half, half)], h_sem.at[i]) for i in range(8)
        ]
        for c in h_copies:
            c.start()

        def x_copies(r, a):
            slot = (z + r + NX - x) % NX
            return [
                pltpu.make_async_copy(
                    x_refs[r * 4 + a * 2 + b],
                    x_s.at[
                        pl.ds(pl.multiple_of(slot * tok, tok), tok),
                        pl.ds(pl.multiple_of((core ^ b) * quarter, quarter), quarter),
                    ],
                    x_sem.at[r, b],
                )
                for b in range(2)
            ]

        for a in range(2):

            @pl.when((yh ^ a) == side)
            def _(a=a):
                for r in range(NX):
                    for c in x_copies(r, a):
                        c.start()

        for c in h_copies:
            c.wait()
        for r in range(NX):
            for c in x_copies(r, 0):
                c.wait()
        for m in range(kinds):
            masked = jnp.where(mod_ref[...] == m, h_s[...], jnp.zeros((), BF))
            o_ref[m] = nn(masked, x_s[...]).astype(dtype)

    return pl.pallas_call(
        body,
        in_specs=[pl.BlockSpec(memory_space=ANY)] * 24 + [pl.BlockSpec(memory_space=VM)],
        out_specs=pl.BlockSpec(memory_space=VM),
        out_shape=jax.ShapeDtypeStruct((kinds, hid, 2 * quarter), dtype),
        scratch_shapes=[
            VM((hid, 8 * half), BF),
            VM((NX * tok, 2 * quarter), BF),
            pltpu.SemaphoreType.DMA((8,)),
            pltpu.SemaphoreType.DMA((NX, 2)),
        ],
        compiler_params=pltpu.CompilerParams(vmem_limit_bytes=LIMIT),
        name="dw_mine" if mine else "dw_sent",
        cost_estimate=pl.CostEstimate(
            flops=2 * kinds * hid * NX * tok * 2 * quarter, bytes_accessed=0, transcendentals=0
        ),
    )(*hid_halves, *pieces, mods)


def finish(gate, up, own, low, high, token_factor):
    tok, hid = gate.shape
    tile = tok // 4

    def body(g_ref, u_ref, own_ref, la, lb, ha, hb, f_ref, gg_ref, ug_ref):
        first = pl.program_id(0) < 2
        low_part = jnp.where(first, la[...], lb[...]).astype(F32)
        high_part = jnp.where(first, ha[...], hb[...]).astype(F32)
        d_t = (own_ref[...] + low_part + high_part) * f_ref[...]
        d = d_t.T
        g = g_ref[...].astype(F32)
        s = jax.nn.sigmoid(g)
        ug_ref[...] = (d * (g * s)).astype(BF)
        gg_ref[...] = (d * u_ref[...].astype(F32) * (s * (1.0 + g * (1.0 - s)))).astype(BF)

    row = pl.BlockSpec((tile, hid), lambda i: (i, 0))
    col = pl.BlockSpec((hid, tile), lambda i: (0, i))
    first = pl.BlockSpec((hid, tile), lambda i: (0, jnp.minimum(i, 1)))
    second = pl.BlockSpec((hid, tile), lambda i: (0, jnp.maximum(i - 2, 0)))
    return pl.pallas_call(
        body,
        grid=(4,),
        in_specs=[row, row, col, first, second, first, second, pl.BlockSpec((1, tile), lambda i: (0, i))],
        out_specs=[row, row],
        out_shape=[jax.ShapeDtypeStruct((tok, hid), BF)] * 2,
        name="finish",
        compiler_params=pltpu.CompilerParams(vmem_limit_bytes=LIMIT),
        cost_estimate=pl.CostEstimate(flops=2_000_000_000, bytes_accessed=8 * tok * hid, transcendentals=0),
    )(gate, up, own, *low, *high, token_factor)


def shards(modality, out_grad, gate_pre, up_pre, down_weight):
    tok = modality.shape[0]
    pairs = [(a * NX + b, b * NX + a) for a in range(NX) for b in range(NX)]
    first = lax.ppermute(out_grad, ("x", "z"), pairs)
    w_other = swapped(down_weight, "yl")
    second = swapped(first, "yh")
    up1, up2 = moved(first, "z", 1), moved(second, "z", 1)
    down1, down2 = moved(first, "z", -1), moved(second, "z", -1)
    far1, far2 = moved(up1, "z", 1), moved(down2, "z", -1)
    pieces = []
    for one, two in ((first, second), (down1, down2), (far1, far2), (up1, up2)):
        pieces += [one, swapped(one, "core"), two, swapped(two, "core")]

    mods = [modality, moved(modality, "x", -1), moved(modality, "x", 2), moved(modality, "x", 1)]
    mods = jnp.concatenate(mods)[None]
    labels = jnp.arange(3, dtype=jnp.int32)
    counts = jnp.sum((mods == labels[:, None]).astype(F32), axis=1)
    counts = counts + swapped(counts, "yl")
    groups = lax.axis_size("x") * lax.axis_size("yl")
    factor = tok * groups / (3.0 * counts)
    own_mod = modality[None]
    token_factor = jnp.where(own_mod == 0, factor[0], jnp.where(own_mod == 1, factor[1], factor[2]))

    h_a = hidden_half(gate_pre, up_pre, 0)
    h_b = hidden_half(gate_pre, up_pre, 1)
    ra, lb = moved(h_a, "x", 1), moved(h_b, "x", -1)
    rb, la = moved(h_b, "x", 1), moved(h_a, "x", -1)
    fa, fb = moved(ra, "x", 1), moved(lb, "x", -1)
    hid_halves = [h_a, h_b, la, lb, fa, fb, ra, rb]

    s2a, s2b = d_hidden_slots(down_weight, w_other, pieces, mods, (2,), "dh_far")
    got_a, got_b = moved(s2a, "x", 1), moved(s2b, "x", -1)
    sent = weight_grad(hid_halves, pieces, mods, False)
    got_dw = swapped(sent, "yl")
    s1a, s1b, s3a, s3b = d_hidden_slots(down_weight, w_other, pieces, mods, (1, 3), "dh_near")
    low_b, high_a = moved(s1b, "x", 1), moved(s3a, "x", -1)
    s1a = (s1a.astype(F32) + got_a.astype(F32)).astype(BF)
    s3b = (s3b.astype(F32) + got_b.astype(F32)).astype(BF)
    low_a, high_b = moved(s1a, "x", 1), moved(s3b, "x", -1)
    (own,) = d_hidden_slots(down_weight, w_other, pieces, mods, (0,), "dh_own")
    mine = weight_grad(hid_halves, pieces, mods, True)
    gate_grad, up_grad = finish(gate_pre, up_pre, own, (low_a, low_b), (high_a, high_b), token_factor)
    down_grad = (mine + got_dw.astype(F32)) * factor[:, None, None]
    return (down_grad, gate_grad, up_grad)


def solution(mesh):
    torus = Mesh(mesh.devices.reshape(4, 2, 4, 2, 2), ("x", "yl", "z", "yh", "core"))
    fsdp = ("x", "yl")
    tensor = ("z", "yh", "core")
    in_specs = (
        P(fsdp),
        P(fsdp, tensor),
        P(fsdp, tensor),
        P(fsdp, tensor),
        P(None, tensor, fsdp),
    )
    out_specs = (P(None, tensor, fsdp), P(fsdp, tensor), P(fsdp, tensor))
    return jax.shard_map(
        shards, mesh=torus, in_specs=in_specs, out_specs=out_specs, check_vma=False
    )
```
